16 devices in a mesh: rep: 1, r: 4 (over y, z), s: 4 (over x, core).
Axes of the slice: x: 2, y: 2, z: 2, core: 2. Of those that a mesh axis runs over, the one named last changes fastest.
Arguments:
- x: bfloat16 [16, 4096, 768], P(('rep', 'r', 's'))
- dy: bfloat16 [16, 4096, 768], P(('rep', 'r', 's'))
- w_gate: bfloat16 [2, 768, 1792], P(None, 's')
- w_up: bfloat16 [2, 768, 1792], P(None, 's')
- w_down: bfloat16 [2, 1792, 768], P(None, 's')
Outputs:
- output 1: bfloat16 [16, 4096, 768], P(('rep', 'r', 's'))
- output 2: bfloat16 [2, 768, 1792], P('rep', 's')
- output 3: bfloat16 [2, 768, 1792], P('rep', 's')
- output 4: bfloat16 [2, 1792, 768], P('rep', 's')
All inputs are finite; a program needn't handle non-finite values.
Results may differ from the reference program's by a relative error of at most 0.018.
Values are sent between devices in bfloat16 or wider.
A program may use at most 2 GiB of HBM per device.

```python
import jax
import jax.numpy as jnp
from jax import lax

SEQUENCES = 16
TOKENS = 4096
D = 768
FF = 1792
LAYERS = 2
NAMES = ("w_gate", "w_up", "w_down")
SHAPES = {"w_gate": (LAYERS, D, FF), "w_up": (LAYERS, D, FF), "w_down": (LAYERS, FF, D)}


def bump(key, n, height):
    away = (jnp.arange(n, dtype=jnp.int32) - jax.random.randint(key, (), 0, n, jnp.int32)) % n
    return jnp.where(away < n // 8, height, 1.0)


def together(key, own, strength):
    shared = jax.random.normal(key, own.shape[1:], jnp.float32)
    return (own + strength * shared) * lax.rsqrt(1 + strength * strength)


def setup_inputs(seed: int = 0, part: int = 0) -> dict:
    kx, kdy, ka, kb, kz, kf, kh, kl, *kw = jax.random.split(jax.random.key(seed), 8 + len(NAMES))
    kx, kdy, ka, kb = (jax.random.fold_in(k, part) for k in (kx, kdy, ka, kb))
    shape = (SEQUENCES, TOKENS, D)
    much_x, much_dy = jax.random.uniform(kz, (2,), jnp.float32, 0.0, 1.0)
    layers = 2.0 ** jax.random.uniform(kl, (LAYERS, 1, 1), jnp.float32, -1.0, 1.0)
    x = together(ka, jax.random.normal(kx, shape, jnp.float32), much_x) * bump(kf, D, 4.0)
    dy = together(kb, jax.random.normal(kdy, shape, jnp.float32), much_dy)
    drawn = {"x": x.astype(jnp.bfloat16), "dy": (dy * (SEQUENCES * TOKENS) ** -0.5).astype(jnp.bfloat16)}
    for key, name in zip(kw, NAMES, strict=True):
        w = jax.random.normal(key, SHAPES[name], jnp.float32) * SHAPES[name][1] ** -0.5
        drawn[name] = (w * {"w_gate": 1.0, "w_up": bump(kh, FF, 4.0), "w_down": layers}[name]).astype(jnp.bfloat16)
    return drawn


def matmul(a, w):
    return jnp.dot(a, w, preferred_element_type=jnp.float32).astype(jnp.bfloat16)


def normed(h):
    wide = h.astype(jnp.float32)
    scale = lax.rsqrt(jnp.mean(wide**2, -1, keepdims=True) + 1e-6)
    return (wide * scale).astype(jnp.bfloat16)


def layer(h, w):
    a = normed(h)
    gate = jnp.dot(a, w["w_gate"], preferred_element_type=jnp.float32)
    up = jnp.dot(a, w["w_up"], preferred_element_type=jnp.float32)
    return h + matmul((jax.nn.silu(gate) * up).astype(jnp.bfloat16), w["w_down"])


def stack(weights, h):
    return lax.scan(lambda h, w: (layer(h, w), None), h, weights)[0]


def reference(x, dy, w_gate, w_up, w_down):
    weights = dict(zip(NAMES, (w_gate, w_up, w_down), strict=True))

    def take(so_far, sequence):
        h, by_y = sequence
        _, back = jax.vjp(stack, weights, h)
        by_weights, by_h = back(by_y)
        return jax.tree.map(lambda total, term: total + term.astype(jnp.float32), so_far, by_weights), by_h

    none_yet = {name: jnp.zeros(w.shape, jnp.float32) for name, w in weights.items()}
    by_weights, by_x = lax.scan(take, none_yet, (x, dy))
    return (by_x, *(by_weights[name].astype(jnp.bfloat16) for name in NAMES))
```

```python
import functools

import jax
import jax.numpy as jnp
from jax import lax
from jax.experimental import pallas as pl
from jax.experimental.pallas import tpu as pltpu
from jax.sharding import PartitionSpec as P

F32, BF = jnp.float32, jnp.bfloat16
NN = (((1,), (0,)), ((), ()))
NT = (((1,), (1,)), ((), ()))
TN = (((0,), (0,)), ((), ()))
ROWS = 512
STRIP = 256
SHARDS = 4


def dot(a, b, dims=NN):
    return lax.dot_general(a, b, dims, preferred_element_type=F32)


def scaled(h):
    wide = h.astype(F32)
    return wide, lax.rsqrt(jnp.mean(wide * wide, -1, keepdims=True) + 1e-6)


def whole(*shape):
    return pl.BlockSpec(shape, lambda i: (0,) * len(shape), pipeline_mode=pl.Buffered(1))


def rows(t, n):
    return pl.BlockSpec((t, n), lambda i: (i, 0))


def cols(n, t):
    return pl.BlockSpec((n, t), lambda i: (0, i))


def out(*shape):
    return jax.ShapeDtypeStruct(shape, BF)


ANY = pl.BlockSpec(memory_space=pl.ANY)


def params(mib=48):
    return pltpu.CompilerParams(vmem_limit_bytes=mib * 2**20, dimension_semantics=("arbitrary",))


class Route:
    def __init__(self, own, dst, send, recv):
        s, r = lax.axis_index("s"), lax.axis_index("r")
        core, z = s % 2, r % 2
        to_x, to_core = {"s": (s + 2) % 4}, {"s": s + 1 - 2 * core}
        to_y, to_z = {"r": (r + 2) % 4}, {"r": r + 1 - 2 * z}
        ry, rz, rd, p = (r + 2) % 4, r + 1 - 2 * z, 3 - r, (s + 2) % 4
        deep, wide = own.shape
        quarter, tile = deep // 4, wide // 128
        cx, cz = 128 * (tile // 3 - tile // 12), 128 * (tile // 3 + tile // 12)
        left, mid, right = pl.ds(0, cx), pl.ds(cx, cz), pl.ds(cx + cz, wide - cx - cz)
        full = pl.ds(0, wide)

        def place(block, q, n=quarter):
            return pl.ds(pl.multiple_of(block * deep + q * quarter, 16), n)

        def mine(q, c):
            return own.at[pl.ds(pl.multiple_of(q * quarter, 16), quarter), c]

        def make(k, src, at, c, to):
            return pltpu.make_async_remote_copy(
                src, dst.at[at, c], send.at[k], recv.at[k], device_id=to, device_id_type=pl.DeviceIdType.MESH
            )

        def on(k, q, c, to):
            at = place(p, q)
            return make(k, dst.at[at, c], at, c, to)

        self.c = [
            make(0, own, place(s, 0, deep), full, to_core),
            make(1, mine(r, full), place(s, r), full, to_x),
            make(2, mine(rd, left), place(s, rd), left, to_x),
            on(3, r, full, to_y),
            on(4, r, full, to_z),
            on(5, r, full, to_core),
            on(6, rd, full, to_core),
            on(7, ry, mid, to_z),
            on(8, rz, right, to_y),
            on(9, ry, full, to_core),
            on(10, rz, full, to_core),
        ]

    def go(self, *which):
        for k in which:
            self.c[k].start()

    def came(self, *which):
        for k in which:
            self.c[k].wait_recv()

    def first(self):
        self.came(1)
        self.go(3, 4, 5)

    def second(self):
        self.came(3)
        self.go(7, 9)
        self.came(4)
        self.go(8, 10)

    def third(self):
        self.came(2, 7, 8)
        self.go(6)

    def rest(self):
        self.came(0, 5, 6, 9, 10)

    def sent(self):
        for copy in self.c:
            copy.wait_send()


def greet():
    s, r = lax.axis_index("s"), lax.axis_index("r")
    barrier = pltpu.get_barrier_semaphore()
    for to in ({"s": (s + 2) % 4}, {"s": s + 1 - 2 * (s % 2)}, {"r": (r + 2) % 4}, {"r": r + 1 - 2 * (r % 2)}):
        pl.semaphore_signal(barrier, 1, device_id=to, device_id_type=pl.DeviceIdType.MESH)
    pl.semaphore_wait(barrier, 4)


def forward_kernel(h, *refs):
    blocks, (y, act, a), given, later, held, own = (
        refs[:3], refs[3:6], refs[6:9], refs[9:12], refs[12:15], refs[15:18]
    )
    near, out_sem, send0, recv0, send1, recv1 = refs[18:]
    i, s = pl.program_id(0), lax.axis_index("s")
    now = [Route(b.at[0], w, send0.at[m], recv0.at[m]) for m, (b, w) in enumerate(zip(blocks, held))]
    then = [Route(b.at[1], w, send1.at[m], recv1.at[m]) for m, (b, w) in enumerate(zip(blocks, later))]

    def spot(w, b):
        deep = b.shape[1]
        return w.at[pl.ds(pl.multiple_of(s * deep, 64), deep)]

    into = [pltpu.make_async_copy(b.at[0], spot(w, b), near.at[0, m]) for m, (b, w) in enumerate(zip(blocks, held))]
    into += [pltpu.make_async_copy(b.at[1], o, near.at[1, m]) for m, (b, o) in enumerate(zip(blocks, own))]
    back = [pltpu.make_async_copy(o, spot(w, b), near.at[2, m]) for m, (b, o, w) in enumerate(zip(blocks, own, later))]
    back += [pltpu.make_async_copy(w, o, out_sem.at[m]) for m, (w, o) in enumerate(zip(held, given))]

    @pl.when(i == 0)
    def _():
        for copy in into:
            copy.start()
        greet()
        for k in (1, 0, 2):
            for route in now:
                route.go(k)
        for route in now:
            route.first()
        for route in now:
            route.second()
        for route in now:
            route.third()
        for route in now:
            route.rest()
        for copy in into:
            copy.wait()
        for copy in back:
            copy.start()
        for k in (1, 0, 2):
            for route in then:
                route.go(k)

    g, u, d = then
    for at, what in enumerate(
        ([g.first], [u.first], [g.second, d.first], [u.second, g.third], [d.second, u.third], [d.third]), 1
    ):

        @pl.when(i == at)
        def _(what=what):
            for stage in what:
                stage()

    forward_body([h], held, [y, act, a])

    @pl.when(i == pl.num_programs(0) - 1)
    def _():
        for route in then:
            route.rest()
        for route in now + then:
            route.sent()
        for copy in back:
            copy.wait()


def forward(h, *blocks):
    n, d = h.shape
    ff = blocks[0].shape[2]
    sizes = [(d, ff), (d, ff), (ff, d)]
    sems = pltpu.SemaphoreType.DMA((3, 11))
    return pl.pallas_call(
        forward_kernel,
        grid=(n // ROWS,),
        in_specs=[rows(ROWS, d)] + [ANY] * 3,
        out_specs=[rows(ROWS, c) for c in (d, ff, d)] + [ANY] * 6,
        out_shape=[out(n, c) for c in (d, ff, d)] + [out(*size) for size in sizes * 2],
        scratch_shapes=[pltpu.VMEM(size, BF) for size in sizes]
        + [pltpu.VMEM(b.shape[1:], BF) for b in blocks]
        + [pltpu.SemaphoreType.DMA((3, 3)), pltpu.SemaphoreType.DMA((3,)), sems, sems, sems, sems],
        compiler_params=pltpu.CompilerParams(
            vmem_limit_bytes=48 * 2**20, dimension_semantics=("arbitrary",), collective_id=0, has_side_effects=True
        ),
        name="forward",
        cost_estimate=pl.CostEstimate(flops=6 * n * d * ff, bytes_accessed=2 * n * (3 * d + ff), transcendentals=n * ff),
    )(h, *blocks)


def forward_body(ins, weights, outs):
    (h_ref,), (wg, wu, wd), (y, act, a_ref) = ins, weights, outs
    h = h_ref[...]
    wide, scale = scaled(h)
    a = (wide * scale).astype(BF)
    a_ref[...] = a
    for f in range(0, wg.shape[1], STRIP):
        cut = slice(f, f + STRIP)
        gate, up = dot(a, wg[:, cut]), dot(a, wu[:, cut])
        act[:, cut] = (jax.nn.silu(gate) * up).astype(BF)
    y[...] = h + dot(act[...], wd[...]).astype(BF)


def middle(h, dy, wg, wu, wd, act, both, a_ref):
    wide, scale = scaled(h)
    a = (wide * scale).astype(BF)
    if a_ref is not None:
        a_ref[...] = a
    ff = wg.shape[1]
    for f in range(0, ff, STRIP):
        cut = slice(f, f + STRIP)
        gate, up = dot(a, wg[:, cut]), dot(a, wu[:, cut])
        by_act = dot(dy, wd[cut, :], NT).astype(BF).astype(F32)
        sig = jax.nn.sigmoid(gate)
        silu = gate * sig
        if act is not None:
            act[:, cut] = (silu * up).astype(BF)
        both[:, cut] = (by_act * up * (sig + silu * (1 - sig))).astype(BF)
        both[:, ff + f : ff + f + STRIP] = (by_act * silu).astype(BF)


def middle_kernel(h, dy, wg, wu, wd, act, both, a):
    middle(h[...], dy[...], wg, wu, wd, act, both, a)


def gradients(h, dy, wg, wu, wd):
    n, d = h.shape
    ff = wg.shape[1]
    return pl.pallas_call(
        middle_kernel,
        grid=(n // ROWS,),
        in_specs=[rows(ROWS, d)] * 2 + [whole(d, ff), whole(d, ff), whole(ff, d)],
        out_specs=[rows(ROWS, c) for c in (ff, 2 * ff, d)],
        out_shape=[out(n, c) for c in (ff, 2 * ff, d)],
        compiler_params=params(),
        name="middle",
        cost_estimate=pl.CostEstimate(flops=6 * n * d * ff, bytes_accessed=2 * n * (3 * d + 3 * ff), transcendentals=n * ff),
    )(h, dy, wg, wu, wd)


def again_kernel(h, dy, wg, wu, wd, both):
    middle(h[...], dy[...], wg, wu, wd, None, both, None)


def again(h, dy, wg, wu, wd):
    n, d = h.shape
    ff = wg.shape[1]
    return pl.pallas_call(
        again_kernel,
        grid=(n // ROWS,),
        in_specs=[rows(ROWS, d)] * 2 + [whole(d, ff), whole(d, ff), whole(ff, d)],
        out_specs=rows(ROWS, 2 * ff),
        out_shape=out(n, 2 * ff),
        compiler_params=params(),
        name="again",
        cost_estimate=pl.CostEstimate(flops=6 * n * d * ff, bytes_accessed=2 * n * (2 * d + 2 * ff), transcendentals=n * ff),
    )(h, dy, wg, wu, wd)


def input_kernel(h, dy, both, wg, wu, o):
    ff = wg.shape[1]
    by_a = (dot(both[:, :ff], wg[...], NT) + dot(both[:, ff:], wu[...], NT)).astype(BF).astype(F32)
    wide, scale = scaled(h[...])
    inner = jnp.mean(by_a * wide, -1, keepdims=True)
    o[...] = dy[...] + (by_a * scale - wide * (scale * scale * scale * inner)).astype(BF)


def by_input(h, dy, both, wg, wu):
    n, d = h.shape
    ff = wg.shape[1]
    return pl.pallas_call(
        input_kernel,
        grid=(n // ROWS,),
        in_specs=[rows(ROWS, d)] * 2 + [rows(ROWS, 2 * ff), whole(d, ff), whole(d, ff)],
        out_specs=rows(ROWS, d),
        out_shape=out(n, d),
        compiler_params=params(),
        name="by_input",
        cost_estimate=pl.CostEstimate(flops=4 * n * d * ff, bytes_accessed=2 * n * (3 * d + 2 * ff), transcendentals=0),
    )(h, dy, both, wg, wu)


def scatter_rows(value, mine, across, give):
    s = lax.axis_index("s")
    deep = value.shape[0] // SHARDS
    for b in range(SHARDS):
        part = value[b * deep : (b + 1) * deep]
        same_core, same_chip = s % 2 == b % 2, s // 2 == b // 2

        @pl.when(same_core & same_chip)
        def _():
            mine[...] = part

        @pl.when(same_core & jnp.logical_not(same_chip))
        def _():
            across[...] = part

        @pl.when(jnp.logical_not(same_core) & same_chip)
        def _():
            give[0] = part

        @pl.when(jnp.logical_not(same_core | same_chip))
        def _():
            give[1] = part


def term_kernel(a, b, mine, across, give):
    scatter_rows(dot(a[...], b[...], TN).astype(BF), mine, across, give)


def term(a, b, width):
    n, d = a.shape
    c = b.shape[1]
    deep = d // SHARDS
    return pl.pallas_call(
        term_kernel,
        grid=(pl.cdiv(c, width),),
        in_specs=[whole(n, d), cols(n, width)],
        out_specs=[cols(deep, width), cols(deep, width), pl.BlockSpec((2, deep, width), lambda i: (0, 0, i))],
        out_shape=[out(deep, c), out(deep, c), out(2, deep, c)],
        compiler_params=params(),
        name="term",
        cost_estimate=pl.CostEstimate(flops=2 * n * d * c, bytes_accessed=2 * n * (d + c), transcendentals=0),
    )(a, b)


def add(*terms):
    return sum(t.astype(F32) for t in terms).astype(BF)


def swapped(v, axis, bit):
    return lax.ppermute(v, axis, [(i, i ^ bit) for i in range(4)])


def summed(parts):
    mine, across, give = parts
    got = swapped(give, "s", 1)
    came = swapped(add(across, got[1]), "s", 2)
    four = add(mine, got[0], came)
    half = four.shape[0] // 2
    first, second = four[:half], four[half:]
    first, second = add(first, swapped(first, "r", 2)), add(second, swapped(second, "r", 1))
    first, second = add(first, swapped(first, "r", 1)), add(second, swapped(second, "r", 2))
    return jnp.concatenate([first, second])


def solution(mesh):
    def step(x, dy, *weights):
        x, dy = x[0], dy[0]
        n, d = x.shape
        ff = weights[0].shape[2]
        h1, act0, a0, *w = forward(x, *weights)
        w0, w1 = w[:3], w[3:]
        act1, both1, a1 = gradients(h1, dy, *w1)
        g1 = [summed(term(act1, dy, STRIP)), summed(term(a1, both1, 512))]
        dy1 = by_input(h1, dy, both1, w1[0], w1[1])
        down0 = summed(term(act0, dy1, STRIP))
        both0 = again(x, dy1, *w0)
        gates0 = summed(term(a0, both0, 512))
        by_x = by_input(x, dy1, both0, w0[0], w0[1])
        gate = jnp.stack([gates0[:, :ff], g1[1][:, :ff]])
        up = jnp.stack([gates0[:, ff:], g1[1][:, ff:]])
        return by_x[None], gate, up, jnp.stack([down0, g1[0]])

    states, cut = P(("rep", "r", "s"), None, None), P(None, "s", None)
    return jax.shard_map(
        step,
        mesh=mesh,
        in_specs=(states, states) + (cut,) * 3,
        out_specs=(states,) + (P("rep", "s", None),) * 3,
        check_vma=False,
    )
```

```python
import functools

import jax
import jax.numpy as jnp
from jax import lax
from jax.experimental import pallas as pl
from jax.experimental.pallas import tpu as pltpu
from jax.sharding import PartitionSpec as P

F32, BF = jnp.float32, jnp.bfloat16
NN = (((1,), (0,)), ((), ()))
NT = (((1,), (1,)), ((), ()))
TN = (((0,), (0,)), ((), ()))
ROWS = 512
STRIP = 256
SHARDS = 4


def dot(a, b, dims=NN):
    return lax.dot_general(a, b, dims, preferred_element_type=F32)


def scaled(h):
    wide = h.astype(F32)
    return wide, lax.rsqrt(jnp.mean(wide * wide, -1, keepdims=True) + 1e-6)


def whole(*shape):
    return pl.BlockSpec(shape, lambda i: (0,) * len(shape), pipeline_mode=pl.Buffered(1))


def rows(t, n):
    return pl.BlockSpec((t, n), lambda i: (i, 0))


def cols(n, t):
    return pl.BlockSpec((n, t), lambda i: (0, i))


def out(*shape):
    return jax.ShapeDtypeStruct(shape, BF)


ANY = pl.BlockSpec(memory_space=pl.ANY)


def params(mib=48):
    return pltpu.CompilerParams(vmem_limit_bytes=mib * 2**20, dimension_semantics=("arbitrary",))


class Route:
    def __init__(self, own, dst, send, recv):
        s, r = lax.axis_index("s"), lax.axis_index("r")
        core, z = s % 2, r % 2
        to_x, to_core = {"s": (s + 2) % 4}, {"s": s + 1 - 2 * core}
        to_y, to_z = {"r": (r + 2) % 4}, {"r": r + 1 - 2 * z}
        ry, rz, rd, p = (r + 2) % 4, r + 1 - 2 * z, 3 - r, (s + 2) % 4
        deep, wide = own.shape
        quarter, tile = deep // 4, wide // 128
        cx, cz = 128 * (tile // 3 - tile // 12), 128 * (tile // 3 + tile // 12)
        left, mid, right = pl.ds(0, cx), pl.ds(cx, cz), pl.ds(cx + cz, wide - cx - cz)
        full = pl.ds(0, wide)

        def place(block, q, n=quarter):
            return pl.ds(pl.multiple_of(block * deep + q * quarter, 16), n)

        def mine(q, c):
            return own.at[pl.ds(pl.multiple_of(q * quarter, 16), quarter), c]

        def make(k, src, at, c, to):
            return pltpu.make_async_remote_copy(
                src, dst.at[at, c], send.at[k], recv.at[k], device_id=to, device_id_type=pl.DeviceIdType.MESH
            )

        def on(k, q, c, to):
            at = place(p, q)
            return make(k, dst.at[at, c], at, c, to)

        self.c = [
            make(0, own, place(s, 0, deep), full, to_core),
            make(1, mine(r, full), place(s, r), full, to_x),
            make(2, mine(rd, left), place(s, rd), left, to_x),
            on(3, r, full, to_y),
            on(4, r, full, to_z),
            on(5, r, full, to_core),
            on(6, rd, full, to_core),
            on(7, ry, mid, to_z),
            on(8, rz, right, to_y),
            on(9, ry, full, to_core),
            on(10, rz, full, to_core),
        ]

    def go(self, *which):
        for k in which:
            self.c[k].start()

    def came(self, *which):
        for k in which:
            self.c[k].wait_recv()

    def first(self):
        self.came(1)
        self.go(3, 4, 5)

    def second(self):
        self.came(3)
        self.go(7, 9)
        self.came(4)
        self.go(8, 10)

    def third(self):
        self.came(2, 7, 8)
        self.go(6)

    def rest(self):
        self.came(0, 5, 6, 9, 10)

    def sent(self):
        for copy in self.c:
            copy.wait_send()


def greet():
    s, r = lax.axis_index("s"), lax.axis_index("r")
    barrier = pltpu.get_barrier_semaphore()
    for to in ({"s": (s + 2) % 4}, {"s": s + 1 - 2 * (s % 2)}, {"r": (r + 2) % 4}, {"r": r + 1 - 2 * (r % 2)}):
        pl.semaphore_signal(barrier, 1, device_id=to, device_id_type=pl.DeviceIdType.MESH)
    pl.semaphore_wait(barrier, 4)


def forward_kernel(h, *refs):
    blocks, (y, act, a), given, later, held, own = (
        refs[:3], refs[3:6], refs[6:9], refs[9:12], refs[12:15], refs[15:18]
    )
    near, out_sem, send0, recv0, send1, recv1 = refs[18:]
    i, s = pl.program_id(0), lax.axis_index("s")
    now = [Route(b.at[0], w, send0.at[m], recv0.at[m]) for m, (b, w) in enumerate(zip(blocks, held))]
    then = [Route(b.at[1], w, send1.at[m], recv1.at[m]) for m, (b, w) in enumerate(zip(blocks, later))]

    def spot(w, b):
        deep = b.shape[1]
        return w.at[pl.ds(pl.multiple_of(s * deep, 64), deep)]

    into = [pltpu.make_async_copy(b.at[0], spot(w, b), near.at[0, m]) for m, (b, w) in enumerate(zip(blocks, held))]
    into += [pltpu.make_async_copy(b.at[1], o, near.at[1, m]) for m, (b, o) in enumerate(zip(blocks, own))]
    back = [pltpu.make_async_copy(o, spot(w, b), near.at[2, m]) for m, (b, o, w) in enumerate(zip(blocks, own, later))]
    back += [pltpu.make_async_copy(w, o, out_sem.at[m]) for m, (w, o) in enumerate(zip(held, given))]

    @pl.when(i == 0)
    def _():
        for copy in into:
            copy.start()
        greet()
        for k in (1, 0, 2):
            for route in now:
                route.go(k)
        for route in now:
            route.first()
        for route in now:
            route.second()
        for route in now:
            route.third()
        for route in now:
            route.rest()
        for copy in into:
            copy.wait()
        for copy in back:
            copy.start()
        for k in (1, 0, 2):
            for route in then:
                route.go(k)

    g, u, d = then
    for at, what in enumerate(
        ([g.first], [u.first], [g.second, d.first], [u.second, g.third], [d.second, u.third], [d.third]), 1
    ):

        @pl.when(i == at)
        def _(what=what):
            for stage in what:
                stage()

    forward_body([h], held, [y, act, a])

    @pl.when(i == pl.num_programs(0) - 1)
    def _():
        for route in then:
            route.rest()
        for route in now + then:
            route.sent()
        for copy in back:
            copy.wait()


def forward(h, *blocks):
    n, d = h.shape
    ff = blocks[0].shape[2]
    sizes = [(d, ff), (d, ff), (ff, d)]
    sems = pltpu.SemaphoreType.DMA((3, 11))
    return pl.pallas_call(
        forward_kernel,
        grid=(n // ROWS,),
        in_specs=[rows(ROWS, d)] + [ANY] * 3,
        out_specs=[rows(ROWS, c) for c in (d, ff, d)] + [ANY] * 6,
        out_shape=[out(n, c) for c in (d, ff, d)] + [out(*size) for size in sizes * 2],
        scratch_shapes=[pltpu.VMEM(size, BF) for size in sizes]
        + [pltpu.VMEM(b.shape[1:], BF) for b in blocks]
        + [pltpu.SemaphoreType.DMA((3, 3)), pltpu.SemaphoreType.DMA((3,)), sems, sems, sems, sems],
        compiler_params=pltpu.CompilerParams(
            vmem_limit_bytes=48 * 2**20, dimension_semantics=("arbitrary",), collective_id=0, has_side_effects=True
        ),
        name="forward",
        cost_estimate=pl.CostEstimate(flops=6 * n * d * ff, bytes_accessed=2 * n * (3 * d + ff), transcendentals=n * ff),
    )(h, *blocks)


def forward_body(ins, weights, outs):
    (h_ref,), (wg, wu, wd), (y, act, a_ref) = ins, weights, outs
    h = h_ref[...]
    wide, scale = scaled(h)
    a = (wide * scale).astype(BF)
    a_ref[...] = a
    for f in range(0, wg.shape[1], STRIP):
        cut = slice(f, f + STRIP)
        gate, up = dot(a, wg[:, cut]), dot(a, wu[:, cut])
        act[:, cut] = (jax.nn.silu(gate) * up).astype(BF)
    y[...] = h + dot(act[...], wd[...]).astype(BF)


def middle(h, dy, wg, wu, wd, act, both, a_ref):
    wide, scale = scaled(h)
    a = (wide * scale).astype(BF)
    if a_ref is not None:
        a_ref[...] = a
    ff = wg.shape[1]
    for f in range(0, ff, STRIP):
        cut = slice(f, f + STRIP)
        gate, up = dot(a, wg[:, cut]), dot(a, wu[:, cut])
        by_act = dot(dy, wd[cut, :], NT).astype(BF).astype(F32)
        sig = jax.nn.sigmoid(gate)
        silu = gate * sig
        if act is not None:
            act[:, cut] = (silu * up).astype(BF)
        both[:, cut] = (by_act * up * (sig + silu * (1 - sig))).astype(BF)
        both[:, ff + f : ff + f + STRIP] = (by_act * silu).astype(BF)


def middle_kernel(h, dy, wg, wu, wd, act, both, a):
    middle(h[...], dy[...], wg, wu, wd, act, both, a)


def gradients(h, dy, wg, wu, wd):
    n, d = h.shape
    ff = wg.shape[1]
    return pl.pallas_call(
        middle_kernel,
        grid=(n // ROWS,),
        in_specs=[rows(ROWS, d)] * 2 + [whole(d, ff), whole(d, ff), whole(ff, d)],
        out_specs=[rows(ROWS, c) for c in (ff, 2 * ff, d)],
        out_shape=[out(n, c) for c in (ff, 2 * ff, d)],
        compiler_params=params(),
        name="middle",
        cost_estimate=pl.CostEstimate(flops=6 * n * d * ff, bytes_accessed=2 * n * (3 * d + 3 * ff), transcendentals=n * ff),
    )(h, dy, wg, wu, wd)


MESH = pl.DeviceIdType.MESH


class Sum:
    def __init__(self, box, got, came, ra, rb, send, recv):
        self.box, self.got, self.came, self.ra, self.rb, self.send, self.recv = box, got, came, ra, rb, send, recv
        s, r = lax.axis_index("s"), lax.axis_index("r")
        self.core, self.x = {"s": s + 1 - 2 * (s % 2)}, {"s": (s + 2) % 4}
        self.y, self.z = {"r": (r + 2) % 4}, {"r": r + 1 - 2 * (r % 2)}
        half = box.shape[2] // 2
        self.top, self.low = pl.ds(0, half), pl.ds(half, half)

    def copy(self, k, j):
        top, low = self.top, self.low
        box, came = self.box, self.came
        src, dst, to = (
            (box.at[j, pl.ds(2, 2)], self.got.at[j], self.core),
            (box.at[j, 1], came.at[j], self.x),
            (box.at[j, 0, top], self.ra.at[j, top], self.y),
            (box.at[j, 0, low], self.ra.at[j, low], self.z),
            (came.at[j, top], self.rb.at[j, top], self.z),
            (came.at[j, low], self.rb.at[j, low], self.y),
        )[k]
        return pltpu.make_async_remote_copy(
            src, dst, self.send.at[k, j], self.recv.at[k, j], device_id=to, device_id_type=MESH
        )

    def cores(self, j):
        self.copy(0, j).start()

    def chips(self, j):
        self.copy(0, j).wait_recv()
        self.box[j, 1] = add(self.box[j, 1], self.got[j, 1])
        self.copy(1, j).start()

    def once(self, j):
        self.copy(1, j).wait_recv()
        self.box[j, 0] = add(self.box[j, 0], self.got[j, 0], self.came[j])
        self.copy(2, j).start()
        self.copy(3, j).start()

    def twice(self, j):
        self.copy(1, j).wait_send()
        self.copy(2, j).wait_recv()
        self.copy(3, j).wait_recv()
        self.came[j] = add(self.box[j, 0], self.ra[j])
        self.copy(4, j).start()
        self.copy(5, j).start()

    def done(self, j):
        self.copy(4, j).wait_recv()
        self.copy(5, j).wait_recv()
        total = add(self.came[j], self.rb[j])
        for k in (0, 2, 3, 4, 5):
            self.copy(k, j).wait_send()
        return total

    @staticmethod
    def scratch(chunks, deep, wide):
        sems = pltpu.SemaphoreType.DMA((6, chunks))
        shape = (chunks, deep, wide)
        return [pltpu.VMEM((chunks, 2, deep, wide), BF)] + [pltpu.VMEM(shape, BF)] * 3 + [sems, sems]


def place_rows(value, box):
    s = lax.axis_index("s")
    deep = value.shape[0] // SHARDS
    for b in range(SHARDS):
        box[2 * ((b % 2 + s % 2) % 2) + (b // 2 + s // 2) % 2] = value[b * deep : (b + 1) * deep]


def hello():
    s, r = lax.axis_index("s"), lax.axis_index("r")
    barrier = pltpu.get_barrier_semaphore()
    for to in ({"s": (s + 2) % 4}, {"s": s + 1 - 2 * (s % 2)}, {"r": (r + 2) % 4}, {"r": r + 1 - 2 * (r % 2)}):
        pl.semaphore_signal(barrier, 1, device_id=to, device_id_type=MESH)


def together():
    pl.semaphore_wait(pltpu.get_barrier_semaphore(), 4)


def add(*terms):
    return sum(t.astype(F32) for t in terms).astype(BF)


def down_kernel(a, b, box):
    place_rows(dot(a[...], b[...], TN).astype(BF), box.at[0])


def down_term(act, dy):
    n, ff = act.shape
    d = dy.shape[1]
    chunks, deep = d // STRIP, ff // SHARDS
    return pl.pallas_call(
        down_kernel,
        grid=(chunks,),
        in_specs=[whole(n, ff), cols(n, STRIP)],
        out_specs=pl.BlockSpec((1, SHARDS, deep, STRIP), lambda i: (i, 0, 0, 0)),
        out_shape=out(chunks, SHARDS, deep, STRIP),
        compiler_params=params(),
        name="down_term",
        cost_estimate=pl.CostEstimate(flops=2 * n * d * ff, bytes_accessed=2 * n * (d + ff), transcendentals=0),
    )(act, dy)


def carry(i, at, total, term, box, sem, result):
    chunks, wide = box.shape[0], box.shape[3]
    load = pltpu.make_async_copy(term, box, sem.at[0])
    begin, chips, once, twice, done = at

    @pl.when(i == begin - 1)
    def _():
        load.start()

    @pl.when(i == begin)
    def _():
        load.wait()
        for j in range(chunks):
            total.cores(j)

    @pl.when(i == chips)
    def _():
        for j in range(chunks):
            total.chips(j)

    for j in range(chunks):
        pl.when(i == once + j)(functools.partial(total.once, j))
        pl.when(i == twice + j)(functools.partial(total.twice, j))
    for j in range(chunks - 1):

        @pl.when(i == done + j)
        def _(j=j):
            result[:, j * wide : (j + 1) * wide] = total.done(j)

    def last():
        j = chunks - 1
        result[:, j * wide : (j + 1) * wide] = total.done(j)

    return last


def again_kernel(h, dy, wg, wu, wd, term, both, result, box, *scratch):
    i = pl.program_id(0)
    total = Sum(box, *scratch[:6])

    @pl.when(i == 0)
    def _():
        hello()

    @pl.when(i == 1)
    def _():
        together()

    last = carry(i, (1, 2, 4, 5, 6), total, term, box, scratch[6], result)
    middle(h[...], dy[...], wg, wu, wd, None, both, None)
    pl.when(i == pl.num_programs(0) - 1)(last)


def carrier(collective_id, mib=60):
    return pltpu.CompilerParams(
        vmem_limit_bytes=mib * 2**20,
        dimension_semantics=("arbitrary",),
        collective_id=collective_id,
        has_side_effects=True,
    )


def again(h, dy, wg, wu, wd, term):
    n, d = h.shape
    ff = wg.shape[1]
    chunks, _, deep, wide = term.shape
    return pl.pallas_call(
        again_kernel,
        grid=(n // ROWS,),
        in_specs=[rows(ROWS, d)] * 2 + [whole(d, ff), whole(d, ff), whole(ff, d), ANY],
        out_specs=[rows(ROWS, 2 * ff), whole(deep, d)],
        out_shape=[out(n, 2 * ff), out(deep, d)],
        scratch_shapes=[pltpu.VMEM(term.shape, BF)] + Sum.scratch(chunks, deep, wide) + [pltpu.SemaphoreType.DMA((1,))],
        compiler_params=carrier(1),
        name="again",
        cost_estimate=pl.CostEstimate(flops=6 * n * d * ff, bytes_accessed=2 * n * (2 * d + 2 * ff), transcendentals=n * ff),
    )(h, dy, wg, wu, wd, term)


def last_kernel(a, side, h, dy, both, wg, wu, *refs, chunks, with_down):
    i = pl.program_id(0)
    if with_down:
        term, o, grad, result, box, *refs = refs
    else:
        o, grad, box, *refs = refs
    total = Sum(box, *refs[:6])
    refs = refs[6:]

    @pl.when(i == 0)
    def _():
        hello()

    @pl.when(i == 1)
    def _():
        together()

    def stage(after, what):
        @pl.when((i >= after) & (i < after + chunks))
        def _():
            what(i - after)

    def finish(j):
        grad[...] = total.done(j)

    stage(8, finish)
    stage(6, total.twice)
    stage(4, total.once)
    stage(2, total.chips)
    stage(1, total.cores)
    if with_down:
        last = carry(i, (2, 9, 11, 12, 13), Sum(refs[0], *refs[1:7]), term, refs[0], refs[7], result)

    @pl.when(i < chunks)
    def _():
        place_rows(dot(a[...], side[...], TN).astype(BF), box.at[i])

    @pl.when(i >= chunks)
    def _():
        input_kernel(h, dy, both, wg, wu, o)

    if with_down:
        pl.when(i == pl.num_programs(0) - 1)(last)


def input_kernel(h, dy, both, wg, wu, o):
    ff = wg.shape[1]
    by_a = (dot(both[:, :ff], wg[...], NT) + dot(both[:, ff:], wu[...], NT)).astype(BF).astype(F32)
    wide, scale = scaled(h[...])
    inner = jnp.mean(by_a * wide, -1, keepdims=True)
    o[...] = dy[...] + (by_a * scale - wide * (scale * scale * scale * inner)).astype(BF)


def last(a, both, h, dy, wg, wu, term, collective_id):
    n, d = h.shape
    ff = wg.shape[1]
    wide = 512
    chunks, deep = 2 * ff // wide, d // SHARDS
    steps = n // ROWS

    def row(c):
        return pl.BlockSpec((ROWS, c), lambda i: (jnp.maximum(i - chunks, 0), 0))

    box = (chunks, SHARDS, deep, wide)
    in_specs = [whole(n, d), pl.BlockSpec((n, wide), lambda i: (0, jnp.minimum(i, chunks - 1)))]
    in_specs += [row(d), row(d), row(2 * ff), whole(d, ff), whole(d, ff)]
    out_specs = [row(d), pl.BlockSpec((deep, wide), lambda i: (0, jnp.clip(i - 8, 0, chunks - 1)))]
    out_shape = [out(n, d), out(deep, 2 * ff)]
    scratch = [pltpu.VMEM(box, BF)] + Sum.scratch(chunks, deep, wide)
    args = [a, both, h, dy, both, wg, wu]
    if term is not None:
        _, _, low, narrow = term.shape
        in_specs.append(ANY)
        args.append(term)
        out_specs.append(whole(low, d))
        out_shape.append(out(low, d))
        scratch += [pltpu.VMEM(term.shape, BF)] + Sum.scratch(term.shape[0], low, narrow)
        scratch += [pltpu.SemaphoreType.DMA((1,))]
    return pl.pallas_call(
        functools.partial(last_kernel, chunks=chunks, with_down=term is not None),
        grid=(chunks + steps,),
        in_specs=in_specs,
        out_specs=out_specs,
        out_shape=out_shape,
        scratch_shapes=scratch,
        compiler_params=carrier(collective_id, 63),
        name="last",
        cost_estimate=pl.CostEstimate(flops=8 * n * d * ff, bytes_accessed=2 * n * (4 * d + 4 * ff), transcendentals=0),
    )(*args)


def solution(mesh):
    def step(x, dy, *weights):
        x, dy = x[0], dy[0]
        n, d = x.shape
        ff = weights[0].shape[2]
        h1, act0, a0, *w = forward(x, *weights)
        w0, w1 = w[:3], w[3:]
        act1, both1, a1 = gradients(h1, dy, *w1)
        dy1, gates1, down1 = last(a1, both1, h1, dy, w1[0], w1[1], down_term(act1, dy), 2)
        both0, down0 = again(x, dy1, *w0, down_term(act0, dy1))
        by_x, gates0 = last(a0, both0, x, dy1, w0[0], w0[1], None, 3)
        gate = jnp.stack([gates0[:, :ff], gates1[:, :ff]])
        up = jnp.stack([gates0[:, ff:], gates1[:, ff:]])
        return by_x[None], gate, up, jnp.stack([down0, down1])

    states, cut = P(("rep", "r", "s"), None, None), P(None, "s", None)
    return jax.shard_map(
        step,
        mesh=mesh,
        in_specs=(states, states) + (cut,) * 3,
        out_specs=(states,) + (P("rep", "s", None),) * 3,
        check_vma=False,
    )
```

```python
import functools

import jax
import jax.numpy as jnp
from jax import lax
from jax.experimental import pallas as pl
from jax.experimental.pallas import tpu as pltpu
from jax.sharding import PartitionSpec as P

F32, BF = jnp.float32, jnp.bfloat16
NN = (((1,), (0,)), ((), ()))
NT = (((1,), (1,)), ((), ()))
TN = (((0,), (0,)), ((), ()))
ROWS = 512
STRIP = 256
SHARDS = 4
MESH = pl.DeviceIdType.MESH


def dot(a, b, dims=NN):
    return lax.dot_general(a, b, dims, preferred_element_type=F32)


def scaled(h):
    wide = h.astype(F32)
    return wide, lax.rsqrt(jnp.mean(wide * wide, -1, keepdims=True) + 1e-6)


def whole(*shape):
    return pl.BlockSpec(shape, lambda i: (0,) * len(shape), pipeline_mode=pl.Buffered(1))


def rows(t, n):
    return pl.BlockSpec((t, n), lambda i: (i, 0))


def cols(n, t):
    return pl.BlockSpec((n, t), lambda i: (0, i))


def out(*shape):
    return jax.ShapeDtypeStruct(shape, BF)


ANY = pl.BlockSpec(memory_space=pl.ANY)


def params(mib=63):
    return pltpu.CompilerParams(vmem_limit_bytes=mib * 2**20, dimension_semantics=("arbitrary",))


class Route:
    def __init__(self, own, dst, lo, wide, send, recv):
        s, r = lax.axis_index("s"), lax.axis_index("r")
        core, z = s % 2, r % 2
        to_x, to_core = {"s": (s + 2) % 4}, {"s": s + 1 - 2 * core}
        to_y, to_z = {"r": (r + 2) % 4}, {"r": r + 1 - 2 * z}
        ry, rz, rd, p = (r + 2) % 4, r + 1 - 2 * z, 3 - r, (s + 2) % 4
        deep = own.shape[0]
        quarter, tile = deep // 4, wide // 128
        cx, cz = 128 * (tile // 3), 128 * ((tile - tile // 3) // 2)
        left, mid, right = pl.ds(lo, cx), pl.ds(lo + cx, cz), pl.ds(lo + cx + cz, wide - cx - cz)
        full = pl.ds(lo, wide)

        def place(block, q, n=quarter):
            return pl.ds(pl.multiple_of(block * deep + q * quarter, 16), n)

        def mine(q, c):
            return own.at[pl.ds(pl.multiple_of(q * quarter, 16), quarter), c]

        def make(k, src, at, c, to):
            return pltpu.make_async_remote_copy(
                src, dst.at[at, c], send.at[k], recv.at[k], device_id=to, device_id_type=pl.DeviceIdType.MESH
            )

        def on(k, q, c, to):
            at = place(p, q)
            return make(k, dst.at[at, c], at, c, to)

        self.c = [
            make(0, own.at[:, full], place(s, 0, deep), full, to_core),
            make(1, mine(r, full), place(s, r), full, to_x),
            make(2, mine(rd, left), place(s, rd), left, to_x),
            on(3, r, full, to_y),
            on(4, r, full, to_z),
            on(5, r, full, to_core),
            on(6, rd, full, to_core),
            on(7, ry, mid, to_z),
            on(8, rz, right, to_y),
            on(9, ry, full, to_core),
            on(10, rz, full, to_core),
        ]

    def go(self, *which):
        for k in which:
            self.c[k].start()

    def came(self, *which):
        for k in which:
            self.c[k].wait_recv()

    def first(self):
        self.came(1)
        self.go(3, 4, 5)

    def second(self):
        self.came(3)
        self.go(7, 9)
        self.came(4)
        self.go(8, 10)

    def third(self):
        self.came(2, 7, 8)
        self.go(6)

    def rest(self):
        self.came(0, 5, 6, 9, 10)

    def sent(self):
        for copy in self.c:
            copy.wait_send()


def hello():
    s, r = lax.axis_index("s"), lax.axis_index("r")
    barrier = pltpu.get_barrier_semaphore()
    for to in ({"s": (s + 2) % 4}, {"s": s + 1 - 2 * (s % 2)}, {"r": (r + 2) % 4}, {"r": r + 1 - 2 * (r % 2)}):
        pl.semaphore_signal(barrier, 1, device_id=to, device_id_type=MESH)


def together():
    pl.semaphore_wait(pltpu.get_barrier_semaphore(), 4)


def forward_kernel(h, *refs):
    blocks, (y, act, a_ref), given, later, held, own = (
        refs[:3], refs[3:6], refs[6:9], refs[9:12], refs[12:15], refs[15:18]
    )
    near, out_sem, send0, recv0, send1, recv1 = refs[18:]
    i, s = pl.program_id(0), lax.axis_index("s")
    wg, wu, wd = held
    ff = wg.shape[1]

    def routes(layer, weights, send, recv):
        return [
            Route(b.at[layer], w, 0, b.shape[2], send.at[m], recv.at[m]) for m, (b, w) in enumerate(zip(blocks, weights))
        ]

    now, then = routes(0, held, send0, recv0), routes(1, later, send1, recv1)
    gates, down = now[:2], now[2]

    def spot(w, b):
        deep = b.shape[1]
        return w.at[pl.ds(pl.multiple_of(s * deep, 64), deep)]

    into = [pltpu.make_async_copy(b.at[0], spot(w, b), near.at[0, m]) for m, (b, w) in enumerate(zip(blocks, held))]
    into += [pltpu.make_async_copy(b.at[1], o, near.at[1, m]) for m, (b, o) in enumerate(zip(blocks, own))]
    back = [pltpu.make_async_copy(o, spot(w, b), near.at[2, m]) for m, (b, o, w) in enumerate(zip(blocks, own, later))]
    back += [pltpu.make_async_copy(w, o, out_sem.at[m]) for m, (w, o) in enumerate(zip(held, given))]

    @pl.when(i == 0)
    def _():
        hello()
        for copy in into:
            copy.start()
        together()
        for k in (1, 2, 0):
            for route in gates:
                route.go(k)
        for k in (1, 2, 0):
            down.go(k)
        for route in gates:
            route.first()
        for route in gates:
            route.second()
        down.first()
        for route in gates:
            route.third()
        for route in gates:
            route.rest()
        for copy in into:
            copy.wait()

    wide, scale = scaled(h[...])
    a = (wide * scale).astype(BF)
    a_ref[...] = a
    for f in range(0, ff, STRIP):
        cut = slice(f, f + STRIP)
        gate, up = dot(a, wg[:, cut]), dot(a, wu[:, cut])
        act[:, cut] = (jax.nn.silu(gate) * up).astype(BF)

    @pl.when(i == 0)
    def _():
        down.second()
        down.third()
        down.rest()
        for k in (1, 2, 0):
            for route in then:
                route.go(k)

    y[...] = h[...] + dot(act[...], wd[...]).astype(BF)
    for m, copy in enumerate(back):
        pl.when(i == m + 1)(copy.start)

    g, u, d = then
    for at, what in enumerate(
        ([g.first], [u.first], [g.second, d.first], [u.second, g.third], [d.second, u.third], [d.third]), 1
    ):

        @pl.when(i == at)
        def _(what=what):
            for stage in what:
                stage()

    @pl.when(i == pl.num_programs(0) - 1)
    def _():
        for route in then:
            route.rest()
        for route in now + then:
            route.sent()
        for copy in back:
            copy.wait()


def forward(h, *blocks):
    n, d = h.shape
    ff = blocks[0].shape[2]
    sizes = [(d, ff), (d, ff), (ff, d)]
    sems = pltpu.SemaphoreType.DMA((3, 11))
    return pl.pallas_call(
        forward_kernel,
        grid=(n // ROWS,),
        in_specs=[rows(ROWS, d)] + [ANY] * 3,
        out_specs=[rows(ROWS, c) for c in (d, ff, d)] + [ANY] * 6,
        out_shape=[out(n, c) for c in (d, ff, d)] + [out(*size) for size in sizes * 2],
        scratch_shapes=[pltpu.VMEM(size, BF) for size in sizes]
        + [pltpu.VMEM(b.shape[1:], BF) for b in blocks]
        + [pltpu.SemaphoreType.DMA((3, 3)), pltpu.SemaphoreType.DMA((3,)), sems, sems, sems, sems],
        compiler_params=carrier(0),
        name="forward",
        cost_estimate=pl.CostEstimate(flops=6 * n * d * ff, bytes_accessed=2 * n * (3 * d + ff), transcendentals=n * ff),
    )(h, *blocks)


def backward(gate, up, by_act, both, at, ff):
    by_act = by_act.astype(BF).astype(F32)
    sig = jax.nn.sigmoid(gate)
    silu = gate * sig
    wide = gate.shape[1]
    both[:, at : at + wide] = (by_act * up * (sig + silu * (1 - sig))).astype(BF)
    both[:, ff + at : ff + at + wide] = (by_act * silu).astype(BF)
    return silu


def accumulate(i, total, act, dy, term):
    total[...] += dot(act, dy, TN)

    @pl.when(i == pl.num_programs(0) - 1)
    def _():
        for j in range(term.shape[0]):
            place_rows(total[:, j * STRIP : (j + 1) * STRIP].astype(BF), term.at[j])


def strips(a, dy, wg, wu, wd, both, act):
    ff = wg.shape[1]
    for f in range(0, ff, STRIP):
        cut = slice(f, f + STRIP)
        gate, up = dot(a, wg[:, cut]), dot(a, wu[:, cut])
        silu = backward(gate, up, dot(dy, wd[cut, :], NT), both, f, ff)
        if act is not None:
            act[:, cut] = (silu * up).astype(BF)


def middle_kernel(h, dy, wg, wu, wd, both, a_ref, term, act, total):
    i = pl.program_id(0)

    @pl.when(i == 0)
    def _():
        total[...] = jnp.zeros_like(total)

    wide, scale = scaled(h[...])
    a = (wide * scale).astype(BF)
    a_ref[...] = a
    strips(a, dy[...], wg, wu, wd, both, act)
    accumulate(i, total, act[...], dy[...], term)


def gradients(h, dy, wg, wu, wd):
    n, d = h.shape
    ff = wg.shape[1]
    term = (d // STRIP, SHARDS, ff // SHARDS, STRIP)
    return pl.pallas_call(
        middle_kernel,
        grid=(n // ROWS,),
        in_specs=[rows(ROWS, d)] * 2 + [whole(d, ff), whole(d, ff), whole(ff, d)],
        out_specs=[rows(ROWS, 2 * ff), rows(ROWS, d), whole(*term)],
        out_shape=[out(n, 2 * ff), out(n, d), out(*term)],
        scratch_shapes=[pltpu.VMEM((ROWS, ff), BF), pltpu.VMEM((ff, d), F32)],
        compiler_params=params(),
        name="middle",
        cost_estimate=pl.CostEstimate(flops=8 * n * d * ff, bytes_accessed=2 * n * (3 * d + 2 * ff), transcendentals=n * ff),
    )(h, dy, wg, wu, wd)


class Sum:
    def __init__(self, box, got, came, ra, rb, send, recv):
        self.box, self.got, self.came, self.ra, self.rb, self.send, self.recv = box, got, came, ra, rb, send, recv
        s, r = lax.axis_index("s"), lax.axis_index("r")
        self.core, self.x = {"s": s + 1 - 2 * (s % 2)}, {"s": (s + 2) % 4}
        self.y, self.z = {"r": (r + 2) % 4}, {"r": r + 1 - 2 * (r % 2)}
        half = box.shape[2] // 2
        self.top, self.low = pl.ds(0, half), pl.ds(half, half)

    def copy(self, k, j):
        top, low = self.top, self.low
        box, came = self.box, self.came
        src, dst, to = (
            (box.at[j, pl.ds(2, 2)], self.got.at[j], self.core),
            (box.at[j, 1], came.at[j], self.x),
            (box.at[j, 0, top], self.ra.at[j, top], self.y),
            (box.at[j, 0, low], self.ra.at[j, low], self.z),
            (came.at[j, top], self.rb.at[j, top], self.z),
            (came.at[j, low], self.rb.at[j, low], self.y),
        )[k]
        return pltpu.make_async_remote_copy(
            src, dst, self.send.at[k, j], self.recv.at[k, j], device_id=to, device_id_type=MESH
        )

    def cores(self, j):
        self.copy(0, j).start()

    def chips(self, j):
        self.copy(0, j).wait_recv()
        self.box[j, 1] = add(self.box[j, 1], self.got[j, 1])
        self.copy(1, j).start()

    def once(self, j):
        self.copy(1, j).wait_recv()
        self.box[j, 0] = add(self.box[j, 0], self.got[j, 0], self.came[j])
        self.copy(2, j).start()
        self.copy(3, j).start()

    def twice(self, j):
        self.copy(1, j).wait_send()
        self.copy(2, j).wait_recv()
        self.copy(3, j).wait_recv()
        self.came[j] = add(self.box[j, 0], self.ra[j])
        self.copy(4, j).start()
        self.copy(5, j).start()

    def done(self, j):
        self.copy(4, j).wait_recv()
        self.copy(5, j).wait_recv()
        total = add(self.came[j], self.rb[j])
        for k in (0, 2, 3, 4, 5):
            self.copy(k, j).wait_send()
        return total

    @staticmethod
    def scratch(chunks, deep, wide):
        sems = pltpu.SemaphoreType.DMA((6, chunks))
        shape = (chunks, deep, wide)
        return [pltpu.VMEM((chunks, 2, deep, wide), BF)] + [pltpu.VMEM(shape, BF)] * 3 + [sems, sems]


def place_rows(value, box):
    s = lax.axis_index("s")
    deep = value.shape[0] // SHARDS
    for b in range(SHARDS):
        box[2 * ((b % 2 + s % 2) % 2) + (b // 2 + s // 2) % 2] = value[b * deep : (b + 1) * deep]


def add(*terms):
    return sum(t.astype(F32) for t in terms).astype(BF)


def carry(i, at, total, term, box, sem, result):
    chunks, wide = box.shape[0], box.shape[3]
    begin, chips, once, twice, done = at
    if term is not None:
        load = pltpu.make_async_copy(term, box, sem.at[0])
        pl.when(i == begin - 1)(load.start)

    @pl.when(i == begin)
    def _():
        if term is not None:
            load.wait()
        for j in range(chunks):
            total.cores(j)

    @pl.when(i == chips)
    def _():
        for j in range(chunks):
            total.chips(j)

    for j in range(chunks):
        pl.when(i == once + j)(functools.partial(total.once, j))
        pl.when(i == twice + j)(functools.partial(total.twice, j))
    for j in range(chunks):

        @pl.when(i == done + j)
        def _(j=j):
            result[:, j * wide : (j + 1) * wide] = total.done(j)


def place_units(value, step, box):
    s = lax.axis_index("s")
    units, per = value.shape[0] // 64, box.shape[2] // 64
    for k in range(units):
        u = step * units + k
        b = u // per
        who = 2 * ((b % 2 + s % 2) % 2) + (b // 2 + s // 2) % 2
        at = pl.ds(pl.multiple_of((u - b * per) * 64, 64), 64)
        for j in range(box.shape[0]):
            box[j, who, at, :] = value[64 * k : 64 * (k + 1), j * STRIP : (j + 1) * STRIP]


def again_kernel(act, all_dy, a, dy, *refs, turns):
    weights, (term, both, result1, result0), held, (sem, box1, box0), scratch = (
        refs[:3], refs[3:7], refs[7:10], refs[10:13], refs[13:]
    )
    i = pl.program_id(0)
    loads = [pltpu.make_async_copy(w, v, sem.at[m]) for m, (w, v) in enumerate(zip(weights, held))]

    @pl.when(i == 1)
    def _():
        for load in loads:
            load.start()

    @pl.when(i == turns)
    def _():
        for load in loads:
            load.wait()

    @pl.when(i == 0)
    def _():
        hello()

    @pl.when(i == 1)
    def _():
        together()

    total1, total0 = Sum(box1, *scratch[:6]), Sum(box0, *scratch[6:12])
    carry(i, (1, 3, turns, turns + 1, turns + 2), total1, term, box1, scratch[12], result1)
    carry(i, (turns, turns + 1, turns + 3, turns + 4, turns + 5), total0, None, box0, None, result0)

    @pl.when(i < turns)
    def _():
        place_units(dot(act[...], all_dy[...], TN).astype(BF), i, box0)

    @pl.when(i >= turns)
    def _():
        strips(a[...], dy[...], *held, both, None)


def carrier(collective_id, mib=63):
    return pltpu.CompilerParams(
        vmem_limit_bytes=mib * 2**20,
        dimension_semantics=("arbitrary",),
        collective_id=collective_id,
        has_side_effects=True,
    )


def again(act, a, dy, wg, wu, wd, term):
    n, d = dy.shape
    ff = act.shape[1]
    chunks, _, deep, wide = term.shape
    turns = ff // STRIP

    def row(c):
        return pl.BlockSpec((ROWS, c), lambda i: (jnp.maximum(i - turns, 0), 0))

    return pl.pallas_call(
        functools.partial(again_kernel, turns=turns),
        grid=(turns + n // ROWS,),
        in_specs=[pl.BlockSpec((n, STRIP), lambda i: (0, jnp.minimum(i, turns - 1))), whole(n, d), row(d), row(d)]
        + [ANY] * 4,
        out_specs=[row(2 * ff), whole(deep, d), whole(deep, d)],
        out_shape=[out(n, 2 * ff), out(deep, d), out(deep, d)],
        scratch_shapes=[pltpu.VMEM((d, ff), BF)] * 2
        + [pltpu.VMEM((ff, d), BF), pltpu.SemaphoreType.DMA((3,))]
        + [pltpu.VMEM(term.shape, BF)] * 2
        + Sum.scratch(chunks, deep, wide) * 2
        + [pltpu.SemaphoreType.DMA((1,))],
        compiler_params=carrier(1),
        name="again",
        cost_estimate=pl.CostEstimate(flops=8 * n * d * ff, bytes_accessed=2 * n * (4 * d + 3 * ff), transcendentals=n * ff),
    )(act, dy, a, dy, wg, wu, wd, term)


def last_kernel(a, side, h, dy, both, *refs, chunks):
    weights, (o, grad), held, (sem, box), refs = refs[:2], refs[2:4], refs[4:6], refs[6:8], refs[8:]
    i = pl.program_id(0)
    total = Sum(box, *refs)
    loads = [pltpu.make_async_copy(w, v, sem.at[m]) for m, (w, v) in enumerate(zip(weights, held))]

    @pl.when(i == 0)
    def _():
        hello()
        for load in loads:
            load.start()

    @pl.when(i == 1)
    def _():
        together()

    @pl.when(i == chunks)
    def _():
        for load in loads:
            load.wait()

    def stage(after, what):
        @pl.when((i >= after) & (i < after + chunks))
        def _():
            what(i - after)

    def finish(j):
        value, per = total.done(j), grad.shape[2] // STRIP
        for k in range(side.shape[1] // STRIP):
            unit = j * (side.shape[1] // STRIP) + k
            which = unit // per
            at = pl.ds(pl.multiple_of((unit - which * per) * STRIP, STRIP), STRIP)
            grad[which, :, at] = value[:, k * STRIP : (k + 1) * STRIP]

    stage(8, finish)
    stage(6, total.twice)
    stage(4, total.once)
    stage(2, total.chips)
    stage(1, total.cores)

    @pl.when(i < chunks)
    def _():
        place_rows(dot(a[...], side[...], TN).astype(BF), box.at[i])

    @pl.when(i >= chunks)
    def _():
        input_kernel(h, dy, both, *held, o)


def input_kernel(h, dy, both, wg, wu, o):
    ff = wg.shape[1]
    by_a = (dot(both[:, :ff], wg[...], NT) + dot(both[:, ff:], wu[...], NT)).astype(BF).astype(F32)
    wide, scale = scaled(h[...])
    inner = jnp.mean(by_a * wide, -1, keepdims=True)
    o[...] = dy[...] + (by_a * scale - wide * (scale * scale * scale * inner)).astype(BF)


def last(a, both, h, dy, wg, wu, collective_id):
    n, d = h.shape
    ff = wg.shape[1]
    wide = 512
    chunks, deep = 2 * ff // wide, d // SHARDS

    def row(c):
        return pl.BlockSpec((ROWS, c), lambda i: (jnp.maximum(i - chunks, 0), 0))

    return pl.pallas_call(
        functools.partial(last_kernel, chunks=chunks),
        grid=(chunks + n // ROWS,),
        in_specs=[whole(n, d), pl.BlockSpec((n, wide), lambda i: (0, jnp.minimum(i, chunks - 1)))]
        + [row(d), row(d), row(2 * ff), ANY, ANY],
        out_specs=[row(d), whole(2, deep, ff)],
        out_shape=[out(n, d), out(2, deep, ff)],
        scratch_shapes=[pltpu.VMEM((d, ff), BF)] * 2
        + [pltpu.SemaphoreType.DMA((2,)), pltpu.VMEM((chunks, SHARDS, deep, wide), BF)]
        + Sum.scratch(chunks, deep, wide),
        compiler_params=carrier(collective_id),
        name="last",
        cost_estimate=pl.CostEstimate(flops=8 * n * d * ff, bytes_accessed=2 * n * (4 * d + 4 * ff), transcendentals=0),
    )(a, both, h, dy, both, wg, wu)


def solution(mesh):
    def step(x, dy, *weights):
        x, dy = x[0], dy[0]
        n, d = x.shape
        ff = weights[0].shape[2]
        h1, act0, a0, *w = forward(x, *weights)
        w0, w1 = w[:3], w[3:]
        both1, a1, term1 = gradients(h1, dy, *w1)
        dy1, gates1 = last(a1, both1, h1, dy, w1[0], w1[1], 2)
        both0, down1, down0 = again(act0, a0, dy1, *w0, term1)
        by_x, gates0 = last(a0, both0, x, dy1, w0[0], w0[1], 3)
        gate, up = (jnp.stack([gates0[k], gates1[k]]) for k in range(2))
        return by_x[None], gate, up, jnp.stack([down0, down1])

    states, cut = P(("rep", "r", "s"), None, None), P(None, "s", None)
    return jax.shard_map(
        step,
        mesh=mesh,
        in_specs=(states, states) + (cut,) * 3,
        out_specs=(states,) + (P("rep", "s", None),) * 3,
        check_vma=False,
    )
```

```python
import functools

import jax
import jax.numpy as jnp
from jax import lax
from jax.experimental import pallas as pl
from jax.experimental.pallas import tpu as pltpu
from jax.sharding import PartitionSpec as P

F32, BF = jnp.float32, jnp.bfloat16
NN = (((1,), (0,)), ((), ()))
NT = (((1,), (1,)), ((), ()))
TN = (((0,), (0,)), ((), ()))
ROWS = 512
STRIP = 256
SHARDS = 4
MESH = pl.DeviceIdType.MESH


def dot(a, b, dims=NN):
    return lax.dot_general(a, b, dims, preferred_element_type=F32)


def scaled(h):
    wide = h.astype(F32)
    return wide, lax.rsqrt(jnp.mean(wide * wide, -1, keepdims=True) + 1e-6)


def whole(*shape):
    return pl.BlockSpec(shape, lambda i: (0,) * len(shape), pipeline_mode=pl.Buffered(1))


def rows(t, n):
    return pl.BlockSpec((t, n), lambda i: (i, 0))


def cols(n, t):
    return pl.BlockSpec((n, t), lambda i: (0, i))


def out(*shape):
    return jax.ShapeDtypeStruct(shape, BF)


ANY = pl.BlockSpec(memory_space=pl.ANY)


def params(mib=63):
    return pltpu.CompilerParams(vmem_limit_bytes=mib * 2**20, dimension_semantics=("arbitrary",))


class Route:
    def __init__(self, own, dst, lo, wide, send, recv):
        s, r = lax.axis_index("s"), lax.axis_index("r")
        core, z = s % 2, r % 2
        to_x, to_core = {"s": (s + 2) % 4}, {"s": s + 1 - 2 * core}
        to_y, to_z = {"r": (r + 2) % 4}, {"r": r + 1 - 2 * z}
        ry, rz, rd, p = (r + 2) % 4, r + 1 - 2 * z, 3 - r, (s + 2) % 4
        deep = own.shape[0]
        quarter, tile = deep // 4, wide // 128
        cx, cz = 128 * (tile // 3), 128 * ((tile - tile // 3) // 2)
        left, mid, right = pl.ds(lo, cx), pl.ds(lo + cx, cz), pl.ds(lo + cx + cz, wide - cx - cz)
        full = pl.ds(lo, wide)

        def place(block, q, n=quarter):
            return pl.ds(pl.multiple_of(block * deep + q * quarter, 16), n)

        def mine(q, c):
            return own.at[pl.ds(pl.multiple_of(q * quarter, 16), quarter), c]

        def make(k, src, at, c, to):
            return pltpu.make_async_remote_copy(
                src, dst.at[at, c], send.at[k], recv.at[k], device_id=to, device_id_type=pl.DeviceIdType.MESH
            )

        def on(k, q, c, to):
            at = place(p, q)
            return make(k, dst.at[at, c], at, c, to)

        self.c = [
            make(0, own.at[:, full], place(s, 0, deep), full, to_core),
            make(1, mine(r, full), place(s, r), full, to_x),
            make(2, mine(rd, left), place(s, rd), left, to_x),
            on(3, r, full, to_y),
            on(4, r, full, to_z),
            on(5, r, full, to_core),
            on(6, rd, full, to_core),
            on(7, ry, mid, to_z),
            on(8, rz, right, to_y),
            on(9, ry, full, to_core),
            on(10, rz, full, to_core),
        ]

    def go(self, *which):
        for k in which:
            self.c[k].start()

    def came(self, *which):
        for k in which:
            self.c[k].wait_recv()

    def first(self):
        self.came(1)
        self.go(3, 4, 5)

    def second(self):
        self.came(3)
        self.go(7, 9)
        self.came(4)
        self.go(8, 10)

    def third(self):
        self.came(2, 7, 8)
        self.go(6)

    def rest(self):
        self.came(0, 5, 6, 9, 10)

    def sent(self):
        for copy in self.c:
            copy.wait_send()


def hello():
    s, r = lax.axis_index("s"), lax.axis_index("r")
    barrier = pltpu.get_barrier_semaphore()
    for to in ({"s": (s + 2) % 4}, {"s": s + 1 - 2 * (s % 2)}, {"r": (r + 2) % 4}, {"r": r + 1 - 2 * (r % 2)}):
        pl.semaphore_signal(barrier, 1, device_id=to, device_id_type=MESH)


def together():
    pl.semaphore_wait(pltpu.get_barrier_semaphore(), 4)


def forward_kernel(h, *refs):
    blocks, (y, act, a_ref), given, later, held, own = (
        refs[:3], refs[3:6], refs[6:9], refs[9:12], refs[12:15], refs[15:18]
    )
    near, out_sem, send0, recv0, send1, recv1 = refs[18:]
    i, s = pl.program_id(0), lax.axis_index("s")
    wg, wu, wd = held
    ff = wg.shape[1]

    def routes(layer, weights, send, recv):
        return [
            Route(b.at[layer], w, 0, b.shape[2], send.at[m], recv.at[m]) for m, (b, w) in enumerate(zip(blocks, weights))
        ]

    now, then = routes(0, held, send0, recv0), routes(1, later, send1, recv1)
    gates, down = now[:2], now[2]

    def spot(w, b):
        deep = b.shape[1]
        return w.at[pl.ds(pl.multiple_of(s * deep, 64), deep)]

    into = [pltpu.make_async_copy(b.at[0], spot(w, b), near.at[0, m]) for m, (b, w) in enumerate(zip(blocks, held))]
    into += [pltpu.make_async_copy(b.at[1], o, near.at[1, m]) for m, (b, o) in enumerate(zip(blocks, own))]
    back = [pltpu.make_async_copy(o, spot(w, b), near.at[2, m]) for m, (b, o, w) in enumerate(zip(blocks, own, later))]
    back += [pltpu.make_async_copy(w, o, out_sem.at[m]) for m, (w, o) in enumerate(zip(held, given))]

    @pl.when(i == 0)
    def _():
        hello()
        for copy in into:
            copy.start()
        together()
        for k in (1, 2, 0):
            for route in gates:
                route.go(k)
        for k in (1, 2, 0):
            down.go(k)
        for route in gates:
            route.first()
        for route in gates:
            route.second()
        down.first()
        for route in gates:
            route.third()
        for route in gates:
            route.rest()
        for copy in into:
            copy.wait()
        down.second()
        down.third()
        down.rest()
        for k in (1, 2, 0):
            for route in then:
                route.go(k)

    wide, scale = scaled(h[...])
    a = (wide * scale).astype(BF)
    a_ref[...] = a
    for f in range(0, ff, STRIP):
        cut = slice(f, f + STRIP)
        gate, up = dot(a, wg[:, cut]), dot(a, wu[:, cut])
        act[:, cut] = (jax.nn.silu(gate) * up).astype(BF)

    y[...] = h[...] + dot(act[...], wd[...]).astype(BF)
    for m, copy in enumerate(back):
        pl.when(i == m + 1)(copy.start)

    g, u, d = then
    for at, what in enumerate(
        ([g.first], [u.first], [g.second, d.first], [u.second, g.third], [d.second, u.third], [d.third]), 1
    ):

        @pl.when(i == at)
        def _(what=what):
            for stage in what:
                stage()

    @pl.when(i == pl.num_programs(0) - 1)
    def _():
        for route in then:
            route.rest()
        for route in now + then:
            route.sent()
        for copy in back:
            copy.wait()


def forward(h, *blocks):
    n, d = h.shape
    ff = blocks[0].shape[2]
    sizes = [(d, ff), (d, ff), (ff, d)]
    sems = pltpu.SemaphoreType.DMA((3, 11))
    return pl.pallas_call(
        forward_kernel,
        grid=(n // ROWS,),
        in_specs=[rows(ROWS, d)] + [ANY] * 3,
        out_specs=[rows(ROWS, c) for c in (d, ff, d)] + [ANY] * 6,
        out_shape=[out(n, c) for c in (d, ff, d)] + [out(*size) for size in sizes * 2],
        scratch_shapes=[pltpu.VMEM(size, BF) for size in sizes]
        + [pltpu.VMEM(b.shape[1:], BF) for b in blocks]
        + [pltpu.SemaphoreType.DMA((3, 3)), pltpu.SemaphoreType.DMA((3,)), sems, sems, sems, sems],
        compiler_params=carrier(0),
        name="forward",
        cost_estimate=pl.CostEstimate(flops=6 * n * d * ff, bytes_accessed=2 * n * (3 * d + ff), transcendentals=n * ff),
    )(h, *blocks)


def backward(gate, up, by_act, both, at, ff):
    by_act = by_act.astype(BF).astype(F32)
    sig = jax.nn.sigmoid(gate)
    silu = gate * sig
    wide = gate.shape[1]
    both[:, at : at + wide] = (by_act * up * (sig + silu * (1 - sig))).astype(BF)
    both[:, ff + at : ff + at + wide] = (by_act * silu).astype(BF)
    return silu


def accumulate(i, total, act, dy, term):
    total[...] += dot(act, dy, TN)

    @pl.when(i == pl.num_programs(0) - 1)
    def _():
        for j in range(term.shape[0]):
            place_rows(total[:, j * STRIP : (j + 1) * STRIP].astype(BF), term.at[j])


def strips(a, dy, wg, wu, wd, both, act):
    ff = wg.shape[1]
    for f in range(0, ff, STRIP):
        cut = slice(f, f + STRIP)
        gate, up = dot(a, wg[:, cut]), dot(a, wu[:, cut])
        silu = backward(gate, up, dot(dy, wd[cut, :], NT), both, f, ff)
        if act is not None:
            act[:, cut] = (silu * up).astype(BF)


def middle_kernel(h, dy, wg, wu, wd, both, a_ref, term, act, total):
    i = pl.program_id(0)

    @pl.when(i == 0)
    def _():
        total[...] = jnp.zeros_like(total)

    wide, scale = scaled(h[...])
    a = (wide * scale).astype(BF)
    a_ref[...] = a
    strips(a, dy[...], wg, wu, wd, both, act)
    accumulate(i, total, act[...], dy[...], term)


def gradients(h, dy, wg, wu, wd):
    n, d = h.shape
    ff = wg.shape[1]
    term = (d // STRIP, SHARDS, ff // SHARDS, STRIP)
    return pl.pallas_call(
        middle_kernel,
        grid=(n // ROWS,),
        in_specs=[rows(ROWS, d)] * 2 + [whole(d, ff), whole(d, ff), whole(ff, d)],
        out_specs=[rows(ROWS, 2 * ff), rows(ROWS, d), whole(*term)],
        out_shape=[out(n, 2 * ff), out(n, d), out(*term)],
        scratch_shapes=[pltpu.VMEM((ROWS, ff), BF), pltpu.VMEM((ff, d), F32)],
        compiler_params=params(),
        name="middle",
        cost_estimate=pl.CostEstimate(flops=8 * n * d * ff, bytes_accessed=2 * n * (3 * d + 2 * ff), transcendentals=n * ff),
    )(h, dy, wg, wu, wd)


class Sum:
    def __init__(self, box, got, came, ra, rb, send, recv):
        self.box, self.got, self.came, self.ra, self.rb, self.send, self.recv = box, got, came, ra, rb, send, recv
        s, r = lax.axis_index("s"), lax.axis_index("r")
        self.core, self.x = {"s": s + 1 - 2 * (s % 2)}, {"s": (s + 2) % 4}
        self.y, self.z = {"r": (r + 2) % 4}, {"r": r + 1 - 2 * (r % 2)}
        half = box.shape[2] // 2
        self.top, self.low = pl.ds(0, half), pl.ds(half, half)

    def copy(self, k, j):
        top, low = self.top, self.low
        box, came = self.box, self.came
        src, dst, to = (
            (box.at[j, pl.ds(2, 2)], self.got.at[j], self.core),
            (box.at[j, 1], came.at[j], self.x),
            (box.at[j, 0, top], self.ra.at[j, top], self.y),
            (box.at[j, 0, low], self.ra.at[j, low], self.z),
            (came.at[j, top], self.rb.at[j, top], self.z),
            (came.at[j, low], self.rb.at[j, low], self.y),
        )[k]
        return pltpu.make_async_remote_copy(
            src, dst, self.send.at[k, j], self.recv.at[k, j], device_id=to, device_id_type=MESH
        )

    def cores(self, j):
        self.copy(0, j).start()

    def chips(self, j):
        self.copy(0, j).wait_recv()
        self.box[j, 1] = add(self.box[j, 1], self.got[j, 1])
        self.copy(1, j).start()

    def once(self, j):
        self.copy(1, j).wait_recv()
        self.box[j, 0] = add(self.box[j, 0], self.got[j, 0], self.came[j])
        self.copy(2, j).start()
        self.copy(3, j).start()

    def twice(self, j):
        self.copy(1, j).wait_send()
        self.copy(2, j).wait_recv()
        self.copy(3, j).wait_recv()
        self.came[j] = add(self.box[j, 0], self.ra[j])
        self.copy(4, j).start()
        self.copy(5, j).start()

    def done(self, j):
        self.copy(4, j).wait_recv()
        self.copy(5, j).wait_recv()
        total = add(self.came[j], self.rb[j])
        for k in (0, 2, 3, 4, 5):
            self.copy(k, j).wait_send()
        return total

    @staticmethod
    def scratch(chunks, deep, wide):
        sems = pltpu.SemaphoreType.DMA((6, chunks))
        shape = (chunks, deep, wide)
        return [pltpu.VMEM((chunks, 2, deep, wide), BF)] + [pltpu.VMEM(shape, BF)] * 3 + [sems, sems]


def place_rows(value, box):
    s = lax.axis_index("s")
    deep = value.shape[0] // SHARDS
    for b in range(SHARDS):
        box[2 * ((b % 2 + s % 2) % 2) + (b // 2 + s // 2) % 2] = value[b * deep : (b + 1) * deep]


def add(*terms):
    return sum(t.astype(F32) for t in terms).astype(BF)


def carry(i, at, total, term, box, sem, result):
    chunks, wide = box.shape[0], box.shape[3]
    begin, chips, once, twice, done = at
    if term is not None:
        load = pltpu.make_async_copy(term, box, sem.at[0])
        pl.when(i == begin - 1)(load.start)

    @pl.when(i == begin)
    def _():
        if term is not None:
            load.wait()
        for j in range(chunks):
            total.cores(j)

    @pl.when(i == chips)
    def _():
        for j in range(chunks):
            total.chips(j)

    for j in range(chunks):
        pl.when(i == once + j)(functools.partial(total.once, j))
        pl.when(i == twice + j)(functools.partial(total.twice, j))
    for j in range(chunks):

        @pl.when(i == done + j)
        def _(j=j):
            result[:, j * wide : (j + 1) * wide] = total.done(j)


def place_units(value, step, box):
    s = lax.axis_index("s")
    units, per = value.shape[0] // 64, box.shape[2] // 64
    for k in range(units):
        u = step * units + k
        b = u // per
        who = 2 * ((b % 2 + s % 2) % 2) + (b // 2 + s // 2) % 2
        at = pl.ds(pl.multiple_of((u - b * per) * 64, 64), 64)
        for j in range(box.shape[0]):
            box[j, who, at, :] = value[64 * k : 64 * (k + 1), j * STRIP : (j + 1) * STRIP]


def again_kernel(act, all_dy, a, dy, *refs, turns):
    weights, (term, both, result1, result0), held, (sem, box1, box0), scratch = (
        refs[:3], refs[3:7], refs[7:10], refs[10:13], refs[13:]
    )
    i = pl.program_id(0)
    loads = [pltpu.make_async_copy(w, v, sem.at[m]) for m, (w, v) in enumerate(zip(weights, held))]

    @pl.when(i == 1)
    def _():
        for load in loads:
            load.start()

    @pl.when(i == turns)
    def _():
        for load in loads:
            load.wait()

    @pl.when(i == 0)
    def _():
        hello()

    @pl.when(i == 1)
    def _():
        together()

    total1, total0 = Sum(box1, *scratch[:6]), Sum(box0, *scratch[6:12])
    carry(i, (1, 3, turns, turns + 1, turns + 2), total1, term, box1, scratch[12], result1)
    carry(i, (turns, turns + 1, turns + 3, turns + 4, turns + 5), total0, None, box0, None, result0)

    @pl.when(i < turns)
    def _():
        place_units(dot(act[...], all_dy[...], TN).astype(BF), i, box0)

    @pl.when(i >= turns)
    def _():
        strips(a[...], dy[...], *held, both, None)


def carrier(collective_id, mib=63):
    return pltpu.CompilerParams(
        vmem_limit_bytes=mib * 2**20,
        dimension_semantics=("arbitrary",),
        collective_id=collective_id,
        has_side_effects=True,
    )


def again(act, a, dy, wg, wu, wd, term):
    n, d = dy.shape
    ff = act.shape[1]
    chunks, _, deep, wide = term.shape
    turns = ff // STRIP

    def row(c):
        return pl.BlockSpec((ROWS, c), lambda i: (jnp.maximum(i - turns, 0), 0))

    return pl.pallas_call(
        functools.partial(again_kernel, turns=turns),
        grid=(turns + n // ROWS,),
        in_specs=[pl.BlockSpec((n, STRIP), lambda i: (0, jnp.minimum(i, turns - 1))), whole(n, d), row(d), row(d)]
        + [ANY] * 4,
        out_specs=[row(2 * ff), whole(deep, d), whole(deep, d)],
        out_shape=[out(n, 2 * ff), out(deep, d), out(deep, d)],
        scratch_shapes=[pltpu.VMEM((d, ff), BF)] * 2
        + [pltpu.VMEM((ff, d), BF), pltpu.SemaphoreType.DMA((3,))]
        + [pltpu.VMEM(term.shape, BF)] * 2
        + Sum.scratch(chunks, deep, wide) * 2
        + [pltpu.SemaphoreType.DMA((1,))],
        compiler_params=carrier(1),
        name="again",
        cost_estimate=pl.CostEstimate(flops=8 * n * d * ff, bytes_accessed=2 * n * (4 * d + 3 * ff), transcendentals=n * ff),
    )(act, dy, a, dy, wg, wu, wd, term)


def last_kernel(a, side, h, dy, both, *refs, chunks):
    weights, (o, grad), held, (sem, box), refs = refs[:2], refs[2:4], refs[4:6], refs[6:8], refs[8:]
    i = pl.program_id(0)
    total = Sum(box, *refs)
    loads = [pltpu.make_async_copy(w, v, sem.at[m]) for m, (w, v) in enumerate(zip(weights, held))]

    @pl.when(i == 0)
    def _():
        hello()
        for load in loads:
            load.start()

    @pl.when(i == 1)
    def _():
        together()

    @pl.when(i == chunks)
    def _():
        for load in loads:
            load.wait()

    def stage(after, what):
        @pl.when((i >= after) & (i < after + chunks))
        def _():
            what(i - after)

    def finish(j):
        value, per = total.done(j), grad.shape[2] // STRIP
        for k in range(side.shape[1] // STRIP):
            unit = j * (side.shape[1] // STRIP) + k
            which = unit // per
            at = pl.ds(pl.multiple_of((unit - which * per) * STRIP, STRIP), STRIP)
            grad[which, :, at] = value[:, k * STRIP : (k + 1) * STRIP]

    stage(8, finish)
    stage(6, total.twice)
    stage(4, total.once)
    stage(2, total.chips)
    stage(1, total.cores)

    @pl.when(i < chunks)
    def _():
        place_rows(dot(a[...], side[...], TN).astype(BF), box.at[i])

    @pl.when(i >= chunks)
    def _():
        input_kernel(h, dy, both, *held, o)


def input_kernel(h, dy, both, wg, wu, o):
    ff = wg.shape[1]
    by_a = (dot(both[:, :ff], wg[...], NT) + dot(both[:, ff:], wu[...], NT)).astype(BF).astype(F32)
    wide, scale = scaled(h[...])
    inner = jnp.mean(by_a * wide, -1, keepdims=True)
    o[...] = dy[...] + (by_a * scale - wide * (scale * scale * scale * inner)).astype(BF)


def last(a, both, h, dy, wg, wu, collective_id):
    n, d = h.shape
    ff = wg.shape[1]
    wide = 512
    chunks, deep = 2 * ff // wide, d // SHARDS

    def row(c):
        return pl.BlockSpec((ROWS, c), lambda i: (jnp.maximum(i - chunks, 0), 0))

    return pl.pallas_call(
        functools.partial(last_kernel, chunks=chunks),
        grid=(chunks + n // ROWS,),
        in_specs=[whole(n, d), pl.BlockSpec((n, wide), lambda i: (0, jnp.minimum(i, chunks - 1)))]
        + [row(d), row(d), row(2 * ff), ANY, ANY],
        out_specs=[row(d), whole(2, deep, ff)],
        out_shape=[out(n, d), out(2, deep, ff)],
        scratch_shapes=[pltpu.VMEM((d, ff), BF)] * 2
        + [pltpu.SemaphoreType.DMA((2,)), pltpu.VMEM((chunks, SHARDS, deep, wide), BF)]
        + Sum.scratch(chunks, deep, wide),
        compiler_params=carrier(collective_id),
        name="last",
        cost_estimate=pl.CostEstimate(flops=8 * n * d * ff, bytes_accessed=2 * n * (4 * d + 4 * ff), transcendentals=0),
    )(a, both, h, dy, both, wg, wu)


def solution(mesh):
    def step(x, dy, *weights):
        x, dy = x[0], dy[0]
        n, d = x.shape
        ff = weights[0].shape[2]
        h1, act0, a0, *w = forward(x, *weights)
        w0, w1 = w[:3], w[3:]
        both1, a1, term1 = gradients(h1, dy, *w1)
        dy1, gates1 = last(a1, both1, h1, dy, w1[0], w1[1], 2)
        both0, down1, down0 = again(act0, a0, dy1, *w0, term1)
        by_x, gates0 = last(a0, both0, x, dy1, w0[0], w0[1], 3)
        gate, up = (jnp.stack([gates0[k], gates1[k]]) for k in range(2))
        return by_x[None], gate, up, jnp.stack([down0, down1])

    states, cut = P(("rep", "r", "s"), None, None), P(None, "s", None)
    return jax.shard_map(
        step,
        mesh=mesh,
        in_specs=(states, states) + (cut,) * 3,
        out_specs=(states,) + (P("rep", "s", None),) * 3,
        check_vma=False,
    )
```
